16 devices in a mesh: pp: 2 (over z), dp: 8 (over y, x, core).
Axes of the slice: x: 2, y: 2, z: 2, core: 2. Of those that a mesh axis runs over, the one named last changes fastest.
Arguments:
- x_in: bfloat16 [4, 16, 128, 1280], P(None, 'dp')
- seed_grad: bfloat16 [4, 16, 128, 1280], P(None, 'dp')
- w_qkv: bfloat16 [4, 1280, 3840], P('pp')
- w_out: bfloat16 [4, 1280, 1280], P('pp')
- w_up: bfloat16 [4, 1280, 5120], P('pp')
- w_down: bfloat16 [4, 5120, 1280], P('pp')
Outputs:
- output 1: bfloat16 [4, 16, 128, 1280], P(None, 'dp')
- output 2: float32 [4, 1280, 3840], P('pp', 'dp')
- output 3: float32 [4, 1280, 1280], P('pp', 'dp')
- output 4: float32 [4, 1280, 5120], P('pp', 'dp')
- output 5: float32 [4, 5120, 1280], P('pp', 'dp')
All inputs are finite; a program needn't handle non-finite values.
Results may differ from the reference program's by a relative error of at most 0.02.
Values are sent between devices in bfloat16 or wider.
A program may use at most 1 GiB of HBM per device.

```python
import jax
import jax.numpy as jnp
from jax import lax

D_MODEL = 1280
HEAD_DIM = 64
LAYERS = 2
MICROBATCHES = 4
BATCH_DEV = 2
SEQ_LEN = 128
STAGES = 2
REPLICAS = 8
NORM_EPS = 1e-6


def setup_inputs(seed: int = 0) -> dict:
    rng_keys = jax.random.split(jax.random.key(seed), 6)
    total_layers = STAGES * LAYERS
    rows_all = REPLICAS * BATCH_DEV
    act_shape = (MICROBATCHES, rows_all, SEQ_LEN, D_MODEL)
    branch = (2.0 * total_layers) ** -0.5
    grad_scale = (MICROBATCHES * rows_all * SEQ_LEN) ** -0.5
    x_in = jax.random.normal(rng_keys[0], act_shape, jnp.float32)
    seed_grad = jax.random.normal(rng_keys[1], act_shape, jnp.float32) * grad_scale
    w_qkv = jax.random.normal(rng_keys[2], (total_layers, D_MODEL, 3 * D_MODEL), jnp.float32) * D_MODEL ** -0.5
    w_out = jax.random.normal(rng_keys[3], (total_layers, D_MODEL, D_MODEL), jnp.float32) * (D_MODEL ** -0.5 * branch)
    w_up = jax.random.normal(rng_keys[4], (total_layers, D_MODEL, 4 * D_MODEL), jnp.float32) * D_MODEL ** -0.5
    w_down = jax.random.normal(rng_keys[5], (total_layers, 4 * D_MODEL, D_MODEL), jnp.float32) * ((4 * D_MODEL) ** -0.5 * branch)
    return {
        "x_in": x_in.astype(jnp.bfloat16),
        "seed_grad": seed_grad.astype(jnp.bfloat16),
        "w_qkv": w_qkv.astype(jnp.bfloat16),
        "w_out": w_out.astype(jnp.bfloat16),
        "w_up": w_up.astype(jnp.bfloat16),
        "w_down": w_down.astype(jnp.bfloat16),
    }


def rms_forward(h_f32):
    return h_f32 * lax.rsqrt(jnp.mean(h_f32 * h_f32, axis=-1, keepdims=True) + NORM_EPS)


def rms_backward(h_f32, grad_f32):
    inv_rms = lax.rsqrt(jnp.mean(h_f32 * h_f32, axis=-1, keepdims=True) + NORM_EPS)
    normed = h_f32 * inv_rms
    return inv_rms * (grad_f32 - normed * jnp.mean(grad_f32 * normed, axis=-1, keepdims=True))


def gelu_tanh(up_f32):
    return jax.nn.gelu(up_f32, approximate=True)


def causal_probs(q_heads, k_heads):
    seq_len = q_heads.shape[1]
    scores = jnp.einsum("bqhe,bkhe->bhqk", q_heads.astype(jnp.float32), k_heads.astype(jnp.float32)) * HEAD_DIM ** -0.5
    allowed = lax.broadcasted_iota(jnp.int32, (seq_len, seq_len), 0) >= lax.broadcasted_iota(jnp.int32, (seq_len, seq_len), 1)
    return jax.nn.softmax(jnp.where(allowed, scores, -1e30), axis=-1)


def layer_forward(h_in, layer_w):
    w_qkv, w_out, w_up, w_down = layer_w
    tokens, model_width = h_in.shape
    head_shape = (tokens // SEQ_LEN, SEQ_LEN, model_width // HEAD_DIM, HEAD_DIM)
    h_f32 = h_in.astype(jnp.float32)
    a_norm = rms_forward(h_f32).astype(jnp.bfloat16)
    qkv_act = jnp.dot(a_norm, w_qkv, preferred_element_type=jnp.float32).astype(jnp.bfloat16)
    q_heads = qkv_act[:, :model_width].reshape(head_shape)
    k_heads = qkv_act[:, model_width:2 * model_width].reshape(head_shape)
    v_heads = qkv_act[:, 2 * model_width:].reshape(head_shape)
    attn_probs = causal_probs(q_heads, k_heads)
    attn_out = jnp.einsum("bhqk,bkhe->bqhe", attn_probs.astype(jnp.bfloat16).astype(jnp.float32), v_heads.astype(jnp.float32)).astype(jnp.bfloat16).reshape(tokens, model_width)
    h_mid = (h_f32 + jnp.dot(attn_out, w_out, preferred_element_type=jnp.float32)).astype(jnp.bfloat16)
    mid_f32 = h_mid.astype(jnp.float32)
    c_norm = rms_forward(mid_f32).astype(jnp.bfloat16)
    up_act = jnp.dot(c_norm, w_up, preferred_element_type=jnp.float32).astype(jnp.bfloat16)
    gelu_act = gelu_tanh(up_act.astype(jnp.float32)).astype(jnp.bfloat16)
    h_out = (mid_f32 + jnp.dot(gelu_act, w_down, preferred_element_type=jnp.float32)).astype(jnp.bfloat16)
    saved_acts = (a_norm, q_heads, k_heads, v_heads, attn_probs, attn_out, h_mid, c_norm, up_act, gelu_act)
    return h_out, saved_acts


def layer_input_grad(d_out, h_in, saved_acts, layer_w):
    w_qkv, w_out, w_up, w_down = layer_w
    a_norm, q_heads, k_heads, v_heads, attn_probs, attn_out, h_mid, c_norm, up_act, gelu_act = saved_acts
    tokens, model_width = d_out.shape
    d_gelu = jnp.dot(d_out, w_down.T, preferred_element_type=jnp.float32)
    gelu_vjp = jax.vjp(gelu_tanh, up_act.astype(jnp.float32))[1]
    d_up = gelu_vjp(d_gelu)[0].astype(jnp.bfloat16)
    d_cnorm = jnp.dot(d_up, w_up.T, preferred_element_type=jnp.float32)
    d_mid = (d_out.astype(jnp.float32) + rms_backward(h_mid.astype(jnp.float32), d_cnorm)).astype(jnp.bfloat16)
    d_attn = jnp.dot(d_mid, w_out.T, preferred_element_type=jnp.float32).astype(jnp.bfloat16).reshape(q_heads.shape)
    d_attn_f32 = d_attn.astype(jnp.float32)
    d_probs = jnp.einsum("bqhe,bkhe->bhqk", d_attn_f32, v_heads.astype(jnp.float32))
    d_vals = jnp.einsum("bhqk,bqhe->bkhe", attn_probs.astype(jnp.bfloat16).astype(jnp.float32), d_attn_f32).astype(jnp.bfloat16)
    d_scores = (attn_probs * (d_probs - jnp.sum(attn_probs * d_probs, axis=-1, keepdims=True)) * HEAD_DIM ** -0.5).astype(jnp.bfloat16)
    d_query = jnp.einsum("bhqk,bkhe->bqhe", d_scores.astype(jnp.float32), k_heads.astype(jnp.float32)).astype(jnp.bfloat16)
    d_key = jnp.einsum("bhqk,bqhe->bkhe", d_scores.astype(jnp.float32), q_heads.astype(jnp.float32)).astype(jnp.bfloat16)
    d_qkv = jnp.concatenate([d_query.reshape(tokens, model_width), d_key.reshape(tokens, model_width), d_vals.reshape(tokens, model_width)], axis=1)
    d_anorm = jnp.dot(d_qkv, w_qkv.T, preferred_element_type=jnp.float32)
    d_in = (d_mid.astype(jnp.float32) + rms_backward(h_in.astype(jnp.float32), d_anorm)).astype(jnp.bfloat16)
    return d_in, (a_norm, d_qkv, attn_out, d_mid, c_norm, d_up, gelu_act, d_out)


def layer_weight_grad(grad_parts):
    a_norm, d_qkv, attn_out, d_mid, c_norm, d_up, gelu_act, d_out = grad_parts
    return (
        jnp.dot(a_norm.T, d_qkv, preferred_element_type=jnp.float32),
        jnp.dot(attn_out.T, d_mid, preferred_element_type=jnp.float32),
        jnp.dot(c_norm.T, d_up, preferred_element_type=jnp.float32),
        jnp.dot(gelu_act.T, d_out, preferred_element_type=jnp.float32),
    )


def reference(x_in, seed_grad, w_qkv, w_out, w_up, w_down):
    num_micro, rows_all, seq_len, model_width = x_in.shape
    tokens = BATCH_DEV * seq_len
    num_chunks = num_micro * rows_all // BATCH_DEV
    x_chunks = x_in.reshape(num_chunks, tokens, model_width)
    g_chunks = seed_grad.reshape(num_chunks, tokens, model_width)
    weights = (w_qkv, w_out, w_up, w_down)

    def forward_layer(h_in, layer_w):
        return layer_forward(h_in, layer_w)[0], h_in

    def backward_layer(d_hid, scan_item):
        h_in, layer_w = scan_item
        saved_acts = layer_forward(h_in, layer_w)[1]
        d_prev, grad_parts = layer_input_grad(d_hid, h_in, saved_acts, layer_w)
        return d_prev, layer_weight_grad(grad_parts)

    def chunk_step(grad_accs, scan_item):
        x_chunk, g_chunk = scan_item
        y_chunk, layer_inputs = lax.scan(forward_layer, x_chunk, weights)
        chunk_grads = lax.scan(backward_layer, g_chunk, (layer_inputs, weights), reverse=True)[1]
        new_accs = tuple(grad_acc + new_grad for grad_acc, new_grad in zip(grad_accs, chunk_grads))
        return new_accs, y_chunk

    zero_accs = tuple(jnp.zeros(weight.shape, jnp.float32) for weight in weights)
    grad_sums, y_chunks = lax.scan(chunk_step, zero_accs, (x_chunks, g_chunks))
    return (y_chunks.reshape(x_in.shape), grad_sums[0], grad_sums[1], grad_sums[2], grad_sums[3])
```

```python
import functools

import jax
import jax.numpy as jnp
from jax import lax
from jax.experimental import pallas as pl
from jax.experimental.pallas import tpu as pltpu
from jax.sharding import PartitionSpec as P

HEAD_DIM = 64
NORM_EPS = 1e-6
GROUP = 2
HID_TILE = 512
HEAD_COLS = 256
SEQ = 128
LANES = 128
F32 = jnp.float32
BF16 = jnp.bfloat16
GELU_A = 0.7978845608028654
GELU_B = 0.044715
VMEM_LIMIT = 56 * 1024 * 1024
TIES = True


def dot_nn(lhs, rhs):
    return lax.dot_general(lhs, rhs, (((1,), (0,)), ((), ())), preferred_element_type=F32)


def dot_nt(lhs, rhs):
    return lax.dot_general(lhs, rhs, (((1,), (1,)), ((), ())), preferred_element_type=F32)


def dot_tn(lhs, rhs):
    return lax.dot_general(lhs, rhs, (((0,), (0,)), ((), ())), preferred_element_type=F32)


def inv_rms_of(h_f32):
    return lax.rsqrt(jnp.mean(h_f32 * h_f32, axis=-1, keepdims=True) + NORM_EPS)


def rms_backward(h_f32, grad_f32):
    inv_rms = inv_rms_of(h_f32)
    normed = h_f32 * inv_rms
    return inv_rms * (grad_f32 - normed * jnp.mean(grad_f32 * normed, axis=-1, keepdims=True))


def head_masks():
    lane = lax.broadcasted_iota(jnp.int32, (1, LANES), 1)
    lo = jnp.where(lane < HEAD_DIM, 1.0, 0.0)
    return lo, 1.0 - lo


def stack_heads(pair, lo, hi):
    return jnp.concatenate([pair * lo.astype(BF16), pair * hi.astype(BF16)], axis=0)


def merge_heads(stacked, lo, hi):
    return stacked[:SEQ] * lo + stacked[SEQ:] * hi


def pair_probs(q_stack, k_pair):
    scores = dot_nt(q_stack, k_pair) * HEAD_DIM ** -0.5
    row = lax.broadcasted_iota(jnp.int32, scores.shape, 0)
    col = lax.broadcasted_iota(jnp.int32, scores.shape, 1)
    scores = jnp.where(jnp.bitwise_and(row, SEQ - 1) >= col, scores, -1e30)
    e = jnp.exp(scores - jnp.max(scores, axis=-1, keepdims=True))
    return e * (1.0 / jnp.sum(e, axis=-1, keepdims=True))


def attn_fwd_kernel(first_layer, n_alias, idx_ref, *refs):
    refs = list(refs)
    if first_layer:
        x_ref, recv_ref = refs[:2]
        refs = refs[2:]
    else:
        h_ref = refs.pop(0)
    wq_ref, wk_ref, wv_ref, wo_ref = refs[:4]
    refs = refs[5 + n_alias:]
    a_out, q_out, k_out, v_out, o_out, h1_out = refs[:6]
    refs = refs[6:]
    if first_layer:
        hin_out = refs.pop(0)
    a_scr, acc = refs
    step = pl.program_id(0)

    @pl.when(step == 0)
    def _():
        if first_layer:
            h_f32 = jnp.where(idx_ref[1] == 1, x_ref[...].astype(F32), recv_ref[...].astype(F32))
            hin_out[...] = h_f32.astype(BF16)
        else:
            h_f32 = h_ref[...].astype(F32)
        a_norm = (h_f32 * inv_rms_of(h_f32)).astype(BF16)
        a_scr[...] = a_norm
        a_out[...] = a_norm
        acc[...] = h_f32

    a_norm = a_scr[...]
    q_out[...] = dot_nn(a_norm, wq_ref[...]).astype(BF16)
    k_out[...] = dot_nn(a_norm, wk_ref[...]).astype(BF16)
    v_out[...] = dot_nn(a_norm, wv_ref[...]).astype(BF16)
    lo, hi = head_masks()
    for seq in range(q_out.shape[0] // SEQ):
        rows = slice(seq * SEQ, (seq + 1) * SEQ)
        for pair in range(HEAD_COLS // LANES):
            cols = slice(pair * LANES, (pair + 1) * LANES)
            probs = pair_probs(stack_heads(q_out[rows, cols], lo, hi), k_out[rows, cols])
            o_stack = dot_nn(probs.astype(BF16), v_out[rows, cols])
            o_out[rows, cols] = merge_heads(o_stack, lo, hi).astype(BF16)
    acc[...] += dot_nn(o_out[...], wo_ref[...])

    @pl.when(step == pl.num_programs(0) - 1)
    def _():
        h1_out[...] = acc[...].astype(BF16)


def ffn_fwd_kernel(last_layer, n_alias, idx_ref, *refs):
    h1_ref, wup_ref, wdown_ref = refs[:3]
    refs = list(refs[3 + n_alias:])
    c_out, u_out, e_out, h2_out = refs[:4]
    refs = refs[4:]
    if last_layer:
        send_out = refs.pop(0)
    c_scr, acc = refs
    step = pl.program_id(0)

    @pl.when(step == 0)
    def _():
        h_f32 = h1_ref[...].astype(F32)
        c_norm = (h_f32 * inv_rms_of(h_f32)).astype(BF16)
        c_scr[...] = c_norm
        c_out[...] = c_norm
        acc[...] = h_f32

    c_norm = c_scr[...]
    for part in range(HID_TILE // 256):
        cols = slice(part * 256, (part + 1) * 256)
        up_act = dot_nn(c_norm, wup_ref[:, cols]).astype(BF16)
        u_out[:, cols] = up_act
        u = up_act.astype(F32)
        gelu = u * (0.5 * (1.0 + jnp.tanh(GELU_A * (u + GELU_B * (u * u * u)))))
        e_out[:, cols] = gelu.astype(BF16)
    acc[...] += dot_nn(e_out[...], wdown_ref[...])

    @pl.when(step == pl.num_programs(0) - 1)
    def _():
        h2 = acc[...].astype(BF16)
        h2_out[...] = h2
        if last_layer:
            send_out[...] = h2


def ffn_bwd_kernel(last_layer, n_alias, idx_ref, *refs):
    refs = list(refs)
    if last_layer:
        seed_ref, recv_ref = refs[:2]
        refs = refs[2:]
    else:
        d_ref = refs.pop(0)
    u_ref, h1_ref, wup_ref, wdown_ref = refs[:4]
    refs = refs[4 + n_alias:]
    du_out, dh1_out = refs[:2]
    refs = refs[2:]
    if last_layer:
        dh2_out = refs.pop(0)
    d_scr, acc = refs
    step = pl.program_id(0)

    @pl.when(step == 0)
    def _():
        if last_layer:
            d_out = jnp.where(idx_ref[1] == 1, seed_ref[...].astype(F32), recv_ref[...].astype(F32)).astype(BF16)
            dh2_out[...] = d_out
        else:
            d_out = d_ref[...]
        d_scr[...] = d_out
        acc[...] = jnp.zeros_like(acc)

    d_out = d_scr[...]
    for part in range(HID_TILE // 256):
        cols = slice(part * 256, (part + 1) * 256)
        d_gelu = dot_nt(d_out, wdown_ref[cols, :])
        u = u_ref[:, cols].astype(F32)
        u2 = u * u
        t = jnp.tanh(GELU_A * (u + GELU_B * (u2 * u)))
        slope = 0.5 * (1.0 + t) + (0.5 * u) * (1.0 - t * t) * (GELU_A + (3.0 * GELU_A * GELU_B) * u2)
        du_out[:, cols] = (d_gelu * slope).astype(BF16)
    acc[...] += dot_nt(du_out[...], wup_ref[...])

    @pl.when(step == pl.num_programs(0) - 1)
    def _():
        back = rms_backward(h1_ref[...].astype(F32), acc[...])
        dh1_out[...] = (d_scr[...].astype(F32) + back).astype(BF16)


def attn_bwd_kernel(first_layer, n_alias, idx_ref, *refs):
    dh1_ref, q_ref, k_ref, v_ref, h_ref, wq_ref, wk_ref, wv_ref, wo_ref = refs[:9]
    dq_out, dk_out, dv_out, dh_out, acc = refs[9 + n_alias:]
    step = pl.program_id(0)

    @pl.when(step == 0)
    def _():
        acc[...] = jnp.zeros_like(acc)

    d_attn = dot_nt(dh1_ref[...], wo_ref[...]).astype(BF16)
    lo, hi = head_masks()
    for seq in range(q_ref.shape[0] // SEQ):
        rows = slice(seq * SEQ, (seq + 1) * SEQ)
        for pair in range(HEAD_COLS // LANES):
            cols = slice(pair * LANES, (pair + 1) * LANES)
            k_pair = k_ref[rows, cols]
            q_stack = stack_heads(q_ref[rows, cols], lo, hi)
            do_stack = stack_heads(d_attn[rows, cols], lo, hi)
            probs = pair_probs(q_stack, k_pair)
            d_probs = dot_nt(do_stack, v_ref[rows, cols])
            row_sum = jnp.sum(probs * d_probs, axis=-1, keepdims=True)
            d_scores = (probs * (d_probs - row_sum) * HEAD_DIM ** -0.5).astype(BF16)
            dq_out[rows, cols] = merge_heads(dot_nn(d_scores, k_pair), lo, hi).astype(BF16)
            dk_out[rows, cols] = dot_tn(d_scores, q_stack).astype(BF16)
            dv_out[rows, cols] = dot_tn(probs.astype(BF16), do_stack).astype(BF16)
    acc[...] += dot_nt(dq_out[...], wq_ref[...]) + dot_nt(dk_out[...], wk_ref[...]) + dot_nt(dv_out[...], wv_ref[...])

    @pl.when(step == pl.num_programs(0) - 1)
    def _():
        back = rms_backward(h_ref[...].astype(F32), acc[...])
        dh_out[...] = (dh1_ref[...].astype(F32) + back).astype(BF16)


def call_slot(body, name, idx, grid, inputs, in_specs, deps, outs, old, scratch, flops):
    any_spec = pl.BlockSpec(memory_space=pl.ANY)
    old = [] if old is None else list(old)
    aliases = {1 + len(inputs) + len(deps) + pos: pos for pos in range(len(old))}
    return pl.pallas_call(
        functools.partial(body, len(old)),
        name=name,
        out_shape=[jax.ShapeDtypeStruct(shape, BF16) for shape, _ in outs],
        grid_spec=pltpu.PrefetchScalarGridSpec(
            num_scalar_prefetch=1,
            grid=(grid,),
            in_specs=list(in_specs) + [any_spec] * (len(deps) + len(old)),
            out_specs=[spec for _, spec in outs],
            scratch_shapes=scratch,
        ),
        input_output_aliases=aliases,
        compiler_params=pltpu.CompilerParams(dimension_semantics=("arbitrary",), vmem_limit_bytes=VMEM_LIMIT),
        cost_estimate=pl.CostEstimate(flops=flops, bytes_accessed=flops // 400, transcendentals=0),
    )(idx, *inputs, *deps, *old)


def solution(mesh):
    assert mesh.shape["pp"] == 2
    num_dp = mesh.shape["dp"]

    def device_step(x_in, seed_grad, w_qkv, w_out, w_up, w_down):
        num_micro, batch_rows, seq_len, width = x_in.shape
        num_layers = w_qkv.shape[0]
        hidden = w_up.shape[2]
        total = num_micro * batch_rows * seq_len
        rows = GROUP * batch_rows * seq_len
        num_groups = num_micro // GROUP
        stage = lax.axis_index("pp")
        x_rows = x_in.reshape(total, width)
        g_rows = seed_grad.reshape(total, width)
        head_steps = width // HEAD_COLS
        hid_steps = hidden // HID_TILE

        whole = lambda step, idx: (idx[0], 0)
        tile = lambda step, idx: (idx[0], step)
        row_spec = pl.BlockSpec((rows, width), whole)
        one_spec = pl.BlockSpec((rows, width), lambda step, idx: (0, 0))
        head_spec = pl.BlockSpec((rows, HEAD_COLS), tile)
        hid_spec = pl.BlockSpec((rows, HID_TILE), tile)
        any_spec = pl.BlockSpec(memory_space=pl.ANY)
        wide = (total, width)
        one = (rows, width)

        def qkv_specs(layer):
            return [
                pl.BlockSpec((None, width, HEAD_COLS), lambda step, idx, third=third: (layer, 0, third * head_steps + step))
                for third in range(3)
            ]

        def wo_spec(layer):
            return pl.BlockSpec((None, HEAD_COLS, width), lambda step, idx: (layer, step, 0))

        def up_spec(layer):
            return pl.BlockSpec((None, width, HID_TILE), lambda step, idx: (layer, 0, step))

        def down_spec(layer):
            return pl.BlockSpec((None, HID_TILE, width), lambda step, idx: (layer, step, 0))

        mat = 2 * rows * width

        def forward(idx, recv, dep, bufs):
            new_bufs = []
            for layer in range(num_layers):
                first, last = layer == 0, layer == num_layers - 1
                old = bufs[layer] if bufs is not None else None
                inputs = [x_rows, recv] if first else [new_bufs[layer - 1]["h2"]]
                in_specs = [row_spec, one_spec] if first else [row_spec]
                names = ["a", "q", "k", "v", "o", "h1"] + (["h"] if first else [])
                specs = [row_spec, head_spec, head_spec, head_spec, head_spec, row_spec] + ([row_spec] if first else [])
                res = call_slot(
                    functools.partial(attn_fwd_kernel, first), f"attn_fwd_{layer}", idx, head_steps,
                    inputs + [w_qkv, w_qkv, w_qkv, w_out], in_specs + qkv_specs(layer) + [wo_spec(layer)], [dep],
                    [(wide, spec) for spec in specs], None if old is None else [old[name] for name in names],
                    [pltpu.VMEM((rows, width), BF16), pltpu.VMEM((rows, width), F32)], 5 * mat * width)
                cur = dict(zip(names, res))
                names = ["c", "u", "e", "h2"]
                hid = (total, hidden)
                outs = [(wide, row_spec), (hid, hid_spec), (hid, hid_spec), (wide, row_spec)]
                if last:
                    outs.append((one, one_spec))
                res = call_slot(
                    functools.partial(ffn_fwd_kernel, last), f"ffn_fwd_{layer}", idx, hid_steps,
                    [cur["h1"], w_up, w_down], [row_spec, up_spec(layer), down_spec(layer)], [],
                    outs, None if old is None else [old[name] for name in names],
                    [pltpu.VMEM((rows, width), BF16), pltpu.VMEM((rows, width), F32)], 2 * mat * hidden)
                cur.update(zip(names, res))
                if not first:
                    cur["h"] = new_bufs[layer - 1]["h2"]
                new_bufs.append(cur)
            return res[4], new_bufs

        def backward(idx, recv, acts, grads):
            new_grads = [{} for _ in range(num_layers)]
            for layer in reversed(range(num_layers)):
                first, last = layer == 0, layer == num_layers - 1
                act, cur = acts[layer], new_grads[layer]
                old = grads[layer] if grads is not None else None
                inputs = [g_rows, recv] if last else [cur["dh2"]]
                in_specs = [row_spec, one_spec] if last else [row_spec]
                names = ["du", "dh1"] + (["dh2"] if last else [])
                outs = [((total, hidden), hid_spec), (wide, row_spec)] + ([(wide, row_spec)] if last else [])
                res = call_slot(
                    functools.partial(ffn_bwd_kernel, last), f"ffn_bwd_{layer}", idx, hid_steps,
                    inputs + [act["u"], act["h1"], w_up, w_down],
                    in_specs + [hid_spec, row_spec, up_spec(layer), down_spec(layer)], [],
                    outs, None if old is None else [old[name] for name in names],
                    [pltpu.VMEM((rows, width), BF16), pltpu.VMEM((rows, width), F32)], 2 * mat * hidden)
                cur.update(zip(names, res))
                names = ["dq", "dk", "dv"]
                olds = None if old is None else [old[name] for name in names]
                outs = [(wide, head_spec)] * 3
                if first:
                    outs = outs + [(one, one_spec)]
                else:
                    outs = outs + [(wide, row_spec)]
                    olds = None if old is None else olds + [grads[layer - 1]["dh2"]]
                res = call_slot(
                    functools.partial(attn_bwd_kernel, first), f"attn_bwd_{layer}", idx, head_steps,
                    [cur["dh1"], act["q"], act["k"], act["v"], act["h"], w_qkv, w_qkv, w_qkv, w_out],
                    [row_spec, head_spec, head_spec, head_spec, row_spec] + qkv_specs(layer) + [wo_spec(layer)], [],
                    outs, olds, [pltpu.VMEM((rows, width), F32)], 5 * mat * width)
                cur.update(zip(names, res))
                if not first:
                    new_grads[layer - 1]["dh2"] = res[3]
            return res[3], new_grads

        def slot_idx(group, flag):
            return jnp.stack([jnp.clip(group, 0, num_groups - 1), flag.astype(jnp.int32)]).astype(jnp.int32)

        recv_fwd = recv_bwd = jnp.zeros(one, BF16)
        acts = grads = None
        dep = recv_fwd
        for tick in range(num_groups + 2):
            if tick <= num_groups:
                send_fwd, acts = forward(slot_idx(tick - stage, stage == 0), recv_fwd, dep, acts)
                if tick < num_groups:
                    recv_fwd = lax.ppermute(send_fwd, "pp", [(0, 1)])
            if tick >= 1:
                send_bwd, grads = backward(slot_idx(tick - 2 + stage, stage == 1), recv_bwd, acts, grads)
                dep = send_bwd
                if tick <= num_groups:
                    recv_bwd = lax.ppermute(send_bwd, "pp", [(1, 0)])

        y_own = acts[-1]["h2"]
        y_recv = lax.ppermute(y_own, "pp", [(1, 0)])
        y_full = jnp.where(stage == 0, y_recv, y_own)

        dp_idx = lax.axis_index("dp")
        core, xpos, ypos = dp_idx % 2, (dp_idx // 2) % 2, dp_idx // 4

        def exchange(value, bit):
            return lax.ppermute(value, "dp", [(i, i ^ bit) for i in range(num_dp)])

        def pick(value, index, axis):
            return lax.dynamic_index_in_dim(value, index, axis, keepdims=False)

        def split_act(act):
            own = act.shape[1] // num_dp
            act_t = act.T.reshape(2, 2, 2, 2, own // 2, total)
            other = pick(act_t, 1 - core, 2)
            kept = pick(act_t, core, 2)
            left, right = kept[:, :, 0], kept[:, :, 1]
            left_x, right_y = pick(left, xpos, 1), pick(right, ypos, 0)
            flat = lambda value: value.reshape(-1, total)
            return {
                "other": flat(other),
                "left_1": flat(pick(left, 1 - xpos, 1)), "right_1": flat(pick(right, 1 - ypos, 0)),
                "left_2": pick(left_x, 1 - ypos, 0), "right_2": pick(right_y, 1 - xpos, 0),
                "final": jnp.concatenate([pick(left_x, ypos, 0), pick(right_y, xpos, 0)], axis=0),
            }

        class Chunk:
            def __init__(self, act, grad):
                self.act, self.grad = act, grad

            def stage_0(self):
                rows_t, grad = self.rows_t, self.grad
                send = dot_nn(rows_t["other"], grad).astype(BF16)
                half, cols = rows_t["left_2"].shape[0], grad.shape[1]
                got = exchange(send, 1).reshape(2, 2, 2, half, cols)
                self.got_left, self.got_right = got[:, :, 0], got[:, :, 1]
                return [send]

            def stage_1(self):
                rows_t, grad = self.rows_t, self.grad
                half, cols = rows_t["left_2"].shape[0], grad.shape[1]
                left = dot_nn(rows_t["left_1"], grad).reshape(2, half, cols)
                left = (left + pick(self.got_left, 1 - xpos, 1).astype(F32)).astype(BF16)
                right = dot_nn(rows_t["right_1"], grad).reshape(2, half, cols)
                right = (right + pick(self.got_right, 1 - ypos, 0).astype(F32)).astype(BF16)
                self.got_left_1, self.got_right_1 = exchange(left, 2), exchange(right, 4)
                self.got_left, self.got_right = pick(self.got_left, xpos, 1), pick(self.got_right, ypos, 0)
                return [left, right]

            def stage_2(self):
                rows_t, grad = self.rows_t, self.grad
                left = dot_nn(rows_t["left_2"], grad)
                left = left + pick(self.got_left, 1 - ypos, 0).astype(F32) + pick(self.got_left_1, 1 - ypos, 0).astype(F32)
                left = left.astype(BF16)
                right = dot_nn(rows_t["right_2"], grad)
                right = right + pick(self.got_right, 1 - xpos, 0).astype(F32) + pick(self.got_right_1, 1 - xpos, 0).astype(F32)
                right = right.astype(BF16)
                self.got_left_2, self.got_right_2 = exchange(left, 4), exchange(right, 2)
                return [left, right]

            def stage_3(self):
                join = lambda left, right: jnp.concatenate([left, right], axis=0).astype(F32)
                out = dot_nn(self.rows_t["final"], self.grad)
                out = out + join(pick(self.got_left, ypos, 0), pick(self.got_right, xpos, 0))
                out = out + join(pick(self.got_left_1, ypos, 0), pick(self.got_right_1, xpos, 0))
                self.out = out + join(self.got_left_2, self.got_right_2)
                return [self.out]

        chunks = []
        for layer in reversed(range(num_layers)):
            act, grad = acts[layer], grads[layer]
            qkv_grad = jnp.concatenate([grad["dq"], grad["dk"], grad["dv"]], axis=1)
            by_name = {"down": Chunk(act["e"], grad["dh2"]), "up": Chunk(act["c"], grad["du"]),
                       "qkv": Chunk(act["a"], qkv_grad), "out": Chunk(act["o"], grad["dh1"])}
            chunks.append(by_name)
        order = [layer[name] for layer in chunks for name in ("down", "up", "qkv", "out")]
        ties = []
        for step in range(len(order) + 3):
            new_ties = []
            if step < len(order):
                chunk = order[step]
                chunk.rows_t = split_act(chunk.act)
                if TIES and ties:
                    chunk.grad = lax.optimization_barrier((chunk.grad, *ties))[0]
                new_ties += chunk.stage_0()
            for lag, name in ((1, "stage_1"), (2, "stage_2"), (3, "stage_3")):
                if 0 <= step - lag < len(order):
                    new_ties += getattr(order[step - lag], name)()
            ties = new_ties
        pieces = [[layer[name].out for layer in reversed(chunks)] for name in ("qkv", "out", "up", "down")]
        grad_outs = [jnp.stack(weight) for weight in pieces]
        return (y_full.reshape(x_in.shape), *grad_outs)

    act_spec = P(None, "dp")
    weight_spec = P("pp")
    grad_spec = P("pp", "dp")
    return jax.shard_map(
        device_step,
        mesh=mesh,
        in_specs=(act_spec, act_spec, weight_spec, weight_spec, weight_spec, weight_spec),
        out_specs=(act_spec, grad_spec, grad_spec, grad_spec, grad_spec),
        check_vma=False,
    )
```

```python
import functools

import jax
import jax.numpy as jnp
from jax import lax
from jax.experimental import pallas as pl
from jax.experimental.pallas import tpu as pltpu
from jax.sharding import PartitionSpec as P

HEAD_DIM = 64
NORM_EPS = 1e-6
GROUP = 2
PARTS = 5
SEQ = 128
LANES = 128
BATCHED = 4
F32 = jnp.float32
BF16 = jnp.bfloat16
GELU_A = 0.7978845608028654
GELU_B = 0.044715
VMEM_LIMIT = 62 * 1024 * 1024


def dot_nn(lhs, rhs):
    return lax.dot_general(lhs, rhs, (((1,), (0,)), ((), ())), preferred_element_type=F32)


def dot_nt(lhs, rhs):
    return lax.dot_general(lhs, rhs, (((1,), (1,)), ((), ())), preferred_element_type=F32)


def dot_tn(lhs, rhs):
    return lax.dot_general(lhs, rhs, (((0,), (0,)), ((), ())), preferred_element_type=F32)


def inv_rms_of(h_f32):
    return lax.rsqrt(jnp.mean(h_f32 * h_f32, axis=-1, keepdims=True) + NORM_EPS)


def rms_backward(h_f32, grad_f32):
    inv_rms = inv_rms_of(h_f32)
    normed = h_f32 * inv_rms
    return inv_rms * (grad_f32 - normed * jnp.mean(grad_f32 * normed, axis=-1, keepdims=True))


def stack_heads(pair):
    lane = lax.broadcasted_iota(jnp.int32, (1, LANES), 1)
    lo = jnp.where(lane < HEAD_DIM, 1.0, 0.0)
    return jnp.concatenate([pair * lo.astype(BF16), pair * (1.0 - lo).astype(BF16)], axis=0)


def merge_heads(stacked):
    lane = lax.broadcasted_iota(jnp.int32, (SEQ, LANES), 1)
    return jnp.where(lane < HEAD_DIM, stacked[:SEQ], stacked[SEQ:])


def probs_of(scores_t):
    key = lax.broadcasted_iota(jnp.int32, scores_t[0].shape, 0)
    query = jnp.bitwise_and(lax.broadcasted_iota(jnp.int32, scores_t[0].shape, 1), SEQ - 1)
    allowed = key <= query
    masked = [jnp.where(allowed, s * HEAD_DIM ** -0.5, -1e30) for s in scores_t]
    tops = [jnp.max(s, axis=0, keepdims=True) for s in masked]
    exps = [jnp.exp(s - top) for s, top in zip(masked, tops)]
    scales = [1.0 / jnp.sum(e, axis=0, keepdims=True) for e in exps]
    return [e * scale for e, scale in zip(exps, scales)]


def batches(num_rows, num_cols):
    combos = [(seq * SEQ, pair * LANES) for seq in range(num_rows // SEQ) for pair in range(num_cols // LANES)]
    return [combos[pos:pos + BATCHED] for pos in range(0, len(combos), BATCHED)]


def cols_of(part, size, base=0):
    return pl.ds(pl.multiple_of(base + part * size, LANES), size)


def fwd_kernel(n_old, names, idx_ref, *refs):
    x_ref, recv_ref, wqkv_ref, wo_ref, wup_ref, wdown_ref = refs[:6]
    refs = list(refs[7 + n_old:])
    outs = {name: refs.pop(0) for name in names}
    send_out = refs.pop(0)
    hacc, big, norm, at_scr, ct_scr, ot_scr, qkv_scr, h_scr, h1_scr, u_scr, et_scr, sems = refs
    rows, width = hacc.shape
    head_cols, hid_cols = width // PARTS, u_scr.shape[1] // PARTS
    layer, step = pl.program_id(0), pl.program_id(1)
    last_layer = pl.num_programs(0) - 1
    row0 = pl.multiple_of(idx_ref[0] * rows, rows)
    sem_of = {name: pos for pos, name in enumerate(names)}

    def whole(name, src, at):
        return pltpu.make_async_copy(src, outs[name].at[at, pl.ds(row0, rows)], sems.at[sem_of[name]])

    def flipped(name, src):
        return pltpu.make_async_copy(src, outs[name].at[layer, idx_ref[0]], sems.at[sem_of[name]])

    def tile(part):
        cols = cols_of(part, hid_cols)
        return pltpu.make_async_copy(u_scr.at[:, cols], outs["u"].at[layer, pl.ds(row0, rows), cols], sems.at[len(names) + 1 + part])

    def again(copy):
        @pl.when(layer > 0)
        def _():
            copy.wait()

    part = lax.rem(step, PARTS)
    phase = step // PARTS

    @pl.when((step == 0) & (layer == 0))
    def _():
        h_f32 = jnp.where(idx_ref[1] == 1, x_ref[...].astype(F32), recv_ref[...].astype(F32))
        h_scr[...] = h_f32.astype(BF16)
        hacc[...] = h_f32
        whole("h", h_scr, 0).start()

    @pl.when(step == 0)
    def _():
        again(flipped("at", at_scr))
        h_f32 = hacc[...]
        norm[...] = (h_f32 * inv_rms_of(h_f32)).astype(BF16)
        big[:, :3 * width] = jnp.zeros((rows, 3 * width), F32)

    @pl.when(phase == 0)
    def _():
        a_cols = norm[:, cols_of(part, head_cols)]
        at_scr[cols_of(part, head_cols), :] = a_cols.T
        big[:, :3 * width] += dot_nn(a_cols, wqkv_ref[...])

    @pl.when(step == PARTS)
    def _():
        again(whole("qkv", qkv_scr, layer))
        again(flipped("ot", ot_scr))
        flipped("at", at_scr).start()
        qkv_scr[...] = big[:, :3 * width].astype(BF16)
        whole("qkv", qkv_scr, layer).start()

    @pl.when(phase == 1)
    def _():
        q = qkv_scr[:, cols_of(part, head_cols)]
        k = qkv_scr[:, cols_of(part, head_cols, width)]
        v = qkv_scr[:, cols_of(part, head_cols, 2 * width)]
        pieces = {}
        for batch in batches(rows, head_cols):
            cut = lambda value: [value[r:r + SEQ, c:c + LANES] for r, c in batch]
            scores = [dot_nt(kp, stack_heads(qp)) for qp, kp in zip(cut(q), cut(k))]
            probs = [p.astype(BF16) for p in probs_of(scores)]
            for at, p, vp in zip(batch, probs, cut(v)):
                pieces[at] = merge_heads(dot_tn(p, vp)).astype(BF16)
        o = jnp.concatenate(
            [jnp.concatenate([pieces[r, c] for c in range(0, head_cols, LANES)], axis=1) for r in range(0, rows, SEQ)], axis=0)
        ot_scr[cols_of(part, head_cols), :] = o.T
        hacc[...] += dot_nn(o, wo_ref[...])

    @pl.when(step == 2 * PARTS - 1)
    def _():
        again(whole("h1", h1_scr, layer))
        flipped("ot", ot_scr).start()
        h1_scr[...] = hacc[...].astype(BF16)
        hacc[...] = h1_scr[...].astype(F32)
        whole("h1", h1_scr, layer).start()

    @pl.when(step == 2 * PARTS)
    def _():
        again(flipped("ct", ct_scr))
        h_f32 = hacc[...]
        norm[...] = (h_f32 * inv_rms_of(h_f32)).astype(BF16)
        big[...] = jnp.zeros_like(big)

    @pl.when(phase == 2)
    def _():
        c_cols = norm[:, cols_of(part, head_cols)]
        ct_scr[cols_of(part, head_cols), :] = c_cols.T
        big[...] += dot_nn(c_cols, wup_ref[...])

    @pl.when(step == 3 * PARTS)
    def _():
        again(flipped("et", et_scr))
        flipped("ct", ct_scr).start()

    @pl.when(phase == 3)
    def _():
        again(tile(part))
        sub = 256
        pieces = []
        for pos in range(hid_cols // sub):
            cols = pl.ds(pl.multiple_of(part * hid_cols + pos * sub, LANES), sub)
            up_act = big[:, cols].astype(BF16)
            u_scr[:, cols] = up_act
            u = up_act.astype(F32)
            gelu = u * (0.5 * (1.0 + jnp.tanh(GELU_A * (u + GELU_B * (u * u * u)))))
            pieces.append(gelu.astype(BF16))
            et_scr[cols, :] = pieces[-1].T
        tile(part).start()
        hacc[...] += dot_nn(jnp.concatenate(pieces, axis=1), wdown_ref[...])

    @pl.when(step == 4 * PARTS - 1)
    def _():
        whole("h", h_scr, 0).wait()
        h_scr[...] = hacc[...].astype(BF16)
        hacc[...] = h_scr[...].astype(F32)
        whole("h", h_scr, layer + 1).start()

        @pl.when(layer < last_layer)
        def _():
            flipped("et", et_scr).start()

        @pl.when(layer == last_layer)
        def _():
            send = pltpu.make_async_copy(h_scr, send_out, sems.at[len(names)])
            send.start()
            flipped("et", et_scr).start()
            for name, src in (("qkv", qkv_scr), ("h1", h1_scr), ("h", h_scr)):
                whole(name, src, layer).wait()
            for name, src in (("at", at_scr), ("ot", ot_scr), ("ct", ct_scr), ("et", et_scr)):
                flipped(name, src).wait()
            for pos in range(PARTS):
                tile(pos).wait()
            send.wait()


def bwd_kernel(top, n_old, names, idx_ref, *refs):
    seed_ref, recv_ref, u_ref, h_any, h1_any, qkv_any, wqkv_ref, wo_ref, wup_ref, wdown_ref = refs[:10]
    refs = list(refs[10 + n_old:])
    outs = {name: refs.pop(0) for name in names}
    send_out = refs.pop(0)
    dacc, d_scr, dh1_scr, du_scr, dqkv_scr, qkv_scr, h_scr, h1_scr, sems, in_sems = refs
    rows, width = dacc.shape
    head_cols, hid_cols = width // PARTS, du_scr.shape[1] // PARTS
    turn, step = pl.program_id(0), pl.program_id(1)
    last_turn = pl.num_programs(0) - 1
    layer = top - turn
    row0 = pl.multiple_of(idx_ref[0] * rows, rows)
    sem_of = {name: pos for pos, name in enumerate(names)}

    def whole(name, src, at):
        return pltpu.make_async_copy(src, outs[name].at[at, pl.ds(row0, rows)], sems.at[sem_of[name]])

    def load(pos, src, dst):
        return pltpu.make_async_copy(src.at[layer, pl.ds(row0, rows)], dst, in_sems.at[pos])

    def again(copy):
        @pl.when(turn > 0)
        def _():
            copy.wait()

    part = lax.rem(step, PARTS)
    phase = step // PARTS

    @pl.when(step == 0)
    def _():
        load(0, h1_any, h1_scr).start()
        load(1, qkv_any, qkv_scr).start()
        load(2, h_any, h_scr).start()

        @pl.when(turn == 0)
        def _():
            seeded = jnp.where(idx_ref[1] == 1, seed_ref[...].astype(F32), recv_ref[...].astype(F32))
            d_scr[...] = seeded.astype(BF16)
            whole("dh2", d_scr, layer).start()

        again(whole("du", du_scr, layer))

    @pl.when(phase == 0)
    def _():
        sub = 256
        d_out = d_scr[...]
        for pos in range(hid_cols // sub):
            d_gelu = dot_nt(d_out, wdown_ref[pos * sub:(pos + 1) * sub, :])
            u = u_ref[:, pos * sub:(pos + 1) * sub].astype(F32)
            u2 = u * u
            t = jnp.tanh(GELU_A * (u + GELU_B * (u2 * u)))
            slope = 0.5 * (1.0 + t) + (0.5 * u) * (1.0 - t * t) * (GELU_A + (3.0 * GELU_A * GELU_B) * u2)
            du_scr[:, pl.ds(pl.multiple_of(part * hid_cols + pos * sub, LANES), sub)] = (d_gelu * slope).astype(BF16)

    @pl.when(step == PARTS)
    def _():
        whole("du", du_scr, layer).start()

    @pl.when(phase == 1)
    def _():
        dacc[:, cols_of(part, width // PARTS)] = dot_nt(du_scr[...], wup_ref[...])

    @pl.when(step == 2 * PARTS - 1)
    def _():
        load(0, h1_any, h1_scr).wait()
        again(whole("dh1", dh1_scr, layer))
        back = rms_backward(h1_scr[...].astype(F32), dacc[...])
        dh1_scr[...] = (d_scr[...].astype(F32) + back).astype(BF16)
        whole("dh1", dh1_scr, layer).start()

    @pl.when(step == 2 * PARTS)
    def _():
        load(1, qkv_any, qkv_scr).wait()
        again(whole("dqkv", dqkv_scr, layer))

    @pl.when(phase == 2)
    def _():
        d_attn = dot_nt(dh1_scr[...], wo_ref[...]).astype(BF16)
        q = qkv_scr[:, cols_of(part, head_cols)]
        k = qkv_scr[:, cols_of(part, head_cols, width)]
        v = qkv_scr[:, cols_of(part, head_cols, 2 * width)]
        pieces = ({}, {}, {})
        for batch in batches(rows, head_cols):
            cut = lambda value: [value[r:r + SEQ, c:c + LANES] for r, c in batch]
            q_stacks = [stack_heads(value) for value in cut(q)]
            do_stacks = [stack_heads(value) for value in cut(d_attn)]
            k_pairs = cut(k)
            probs = probs_of([dot_nt(kp, qs) for kp, qs in zip(k_pairs, q_stacks)])
            d_probs = [dot_nt(vp, ds) for vp, ds in zip(cut(v), do_stacks)]
            sums = [jnp.sum(p * dp, axis=0, keepdims=True) for p, dp in zip(probs, d_probs)]
            d_scores = [(p * (dp - s) * HEAD_DIM ** -0.5).astype(BF16) for p, dp, s in zip(probs, d_probs, sums)]
            for pos, at in enumerate(batch):
                pieces[0][at] = merge_heads(dot_tn(d_scores[pos], k_pairs[pos])).astype(BF16)
                pieces[1][at] = dot_nn(d_scores[pos], q_stacks[pos]).astype(BF16)
                pieces[2][at] = dot_nn(probs[pos].astype(BF16), do_stacks[pos]).astype(BF16)
        for third in range(3):
            dqkv_scr[:, cols_of(part, head_cols, third * width)] = jnp.concatenate(
                [jnp.concatenate([pieces[third][r, c] for c in range(0, head_cols, LANES)], axis=1) for r in range(0, rows, SEQ)], axis=0)

    @pl.when(step == 3 * PARTS)
    def _():
        whole("dqkv", dqkv_scr, layer).start()

    @pl.when(phase == 3)
    def _():
        dacc[:, cols_of(part, width // PARTS)] = dot_nt(dqkv_scr[...], wqkv_ref[...])

    @pl.when(step == 4 * PARTS - 1)
    def _():
        load(2, h_any, h_scr).wait()

        @pl.when(turn == 0)
        def _():
            whole("dh2", d_scr, layer).wait()

        back = rms_backward(h_scr[...].astype(F32), dacc[...])
        d_scr[...] = (dh1_scr[...].astype(F32) + back).astype(BF16)

        @pl.when(turn < last_turn)
        def _():
            copy = whole("dh2", d_scr, layer - 1)
            copy.start()
            copy.wait()

        @pl.when(turn == last_turn)
        def _():
            send = pltpu.make_async_copy(d_scr, send_out, sems.at[len(names)])
            send.start()
            for name, src in (("du", du_scr), ("dh1", dh1_scr), ("dqkv", dqkv_scr)):
                whole(name, src, layer).wait()
            send.wait()


def hold(phase, top):
    def index(turn, step, idx):
        part = jnp.clip(step - phase * PARTS, 0, PARTS - 1)
        before = (step < phase * PARTS) & (turn > 0)
        turn = jnp.where(before, turn - 1, turn)
        part = jnp.where(before, PARTS - 1, part)
        return (turn if top is None else top - turn), part
    return index


def wgrad_kernel(n_deps, n_pairs, has_all, two_outs, idx_ref, lhs_ref, rhs_ref, *refs):
    refs = list(refs)
    all_ref = refs.pop(0) if has_all else None
    pairs = [(refs.pop(0), refs.pop(0)) for _ in range(n_pairs)]
    refs = refs[n_deps:]
    is_left = pl.program_id(0) == 0
    lhs = jnp.concatenate([lhs_ref[group] for group in range(lhs_ref.shape[0])], axis=1)
    out = dot_nn(lhs, rhs_ref[...])
    if has_all:
        out = out + all_ref[...].astype(F32)

    def finish(side):
        done = out
        for pair in pairs:
            done = done + pair[side][...].astype(F32)
        out_ref = refs[side if two_outs else 0]
        out_ref[...] = done.astype(out_ref.dtype)

    if pairs or two_outs:
        pl.when(is_left)(lambda: finish(0))
        pl.when(jnp.logical_not(is_left))(lambda: finish(1))
    else:
        finish(0)


def solution(mesh):
    assert mesh.shape["pp"] == 2
    num_dp = mesh.shape["dp"]

    def device_step(x_in, seed_grad, w_qkv, w_out, w_up, w_down):
        num_micro, batch_rows, seq_len, width = x_in.shape
        num_layers = w_qkv.shape[0]
        hidden = w_up.shape[2]
        total = num_micro * batch_rows * seq_len
        rows = GROUP * batch_rows * seq_len
        num_groups = num_micro // GROUP
        stage = lax.axis_index("pp")
        x_rows = x_in.reshape(total, width)
        g_rows = seed_grad.reshape(total, width)
        any_spec = pl.BlockSpec(memory_space=pl.ANY)
        row_spec = pl.BlockSpec((rows, width), lambda turn, step, idx: (idx[0], 0))
        one_spec = pl.BlockSpec((rows, width), lambda turn, step, idx: (0, 0))
        one = jax.ShapeDtypeStruct((rows, width), BF16)

        def array(*shape):
            return jax.ShapeDtypeStruct(shape, BF16)

        def weight_spec(weight, phase, top):
            index = hold(phase, top)
            return pl.BlockSpec((None, weight.shape[1] // PARTS, weight.shape[2]), lambda turn, step, idx: (*index(turn, step, idx), 0))

        def slot_call(body, name, turns, idx, inputs, in_specs, old, names, shapes, scratch):
            old = [] if old is None else [old[key] for key in names]
            res = pl.pallas_call(
                functools.partial(body, len(old), names),
                name=name,
                out_shape=[shapes[key] for key in names] + [one],
                grid_spec=pltpu.PrefetchScalarGridSpec(
                    num_scalar_prefetch=1,
                    grid=(turns, 4 * PARTS),
                    in_specs=in_specs + [any_spec] * len(old),
                    out_specs=[any_spec] * (len(names) + 1),
                    scratch_shapes=scratch,
                ),
                input_output_aliases={1 + len(inputs) + pos: pos for pos in range(len(old))},
                compiler_params=pltpu.CompilerParams(
                    dimension_semantics=("arbitrary", "arbitrary"), vmem_limit_bytes=VMEM_LIMIT),
                cost_estimate=pl.CostEstimate(
                    flops=turns * 24 * rows * width * width, bytes_accessed=turns * 40 * width * width, transcendentals=0),
            )(idx, *inputs, *old)
            return res[-1], dict(zip(names, res))

        vmem = lambda *shape: pltpu.VMEM(shape, BF16)
        fwd_shapes = {
            "h": array(num_layers + 1, total, width), "at": array(num_layers, num_groups, width, rows),
            "qkv": array(num_layers, total, 3 * width), "ot": array(num_layers, num_groups, width, rows),
            "h1": array(num_layers, total, width), "ct": array(num_layers, num_groups, width, rows),
            "u": array(num_layers, total, hidden), "et": array(num_layers, num_groups, hidden, rows),
        }
        bwd_shapes = {
            "dh2": array(num_layers, total, width), "du": array(num_layers, total, hidden),
            "dh1": array(num_layers, total, width), "dqkv": array(num_layers, total, 3 * width),
        }

        def forward(idx, recv, dep, old):
            inputs = [x_rows, recv, w_qkv, w_out, w_up, w_down, dep]
            in_specs = [row_spec, one_spec] + [weight_spec(weight, phase, None) for phase, weight in enumerate(inputs[2:6])] + [any_spec]
            scratch = [
                pltpu.VMEM((rows, width), F32), pltpu.VMEM((rows, hidden), F32), vmem(rows, width), vmem(width, rows),
                vmem(width, rows), vmem(width, rows), vmem(rows, 3 * width), vmem(rows, width), vmem(rows, width),
                vmem(rows, hidden), vmem(hidden, rows), pltpu.SemaphoreType.DMA((len(fwd_shapes) + 1 + PARTS,)),
            ]
            return slot_call(fwd_kernel, "stage_fwd", num_layers, idx, inputs, in_specs, old, tuple(fwd_shapes), fwd_shapes, scratch)

        def backward(idx, recv, act, old, top, turns):
            inputs = [g_rows, recv, act["u"], act["h"], act["h1"], act["qkv"], w_qkv, w_out, w_up, w_down]
            u_index = hold(0, top)

            def u_block(turn, step, idx):
                layer, part = u_index(turn, step, idx)
                return layer, idx[0], part

            in_specs = [row_spec, one_spec, pl.BlockSpec((None, rows, hidden // PARTS), u_block), any_spec, any_spec, any_spec]
            in_specs += [weight_spec(weight, phase, top) for weight, phase in zip(inputs[6:], (3, 2, 1, 0))]
            scratch = [
                pltpu.VMEM((rows, width), F32), vmem(rows, width), vmem(rows, width), vmem(rows, hidden), vmem(rows, 3 * width),
                vmem(rows, 3 * width), vmem(rows, width), vmem(rows, width),
                pltpu.SemaphoreType.DMA((len(bwd_shapes) + 1,)), pltpu.SemaphoreType.DMA((3,)),
            ]
            return slot_call(functools.partial(bwd_kernel, top), f"stage_bwd_{top}", turns, idx, inputs, in_specs, old,
                             tuple(bwd_shapes), bwd_shapes, scratch)

        def slot_idx(group, flag):
            return jnp.stack([jnp.clip(group, 0, num_groups - 1), flag.astype(jnp.int32)]).astype(jnp.int32)

        dp_idx = lax.axis_index("dp")
        core, xpos, ypos = dp_idx % 2, (dp_idx // 2) % 2, dp_idx // 4
        place = lambda y, x: 2 * y + x
        picks = {
            0: [place(0, 0), place(0, 1), place(1, 0), place(1, 1)] * 2,
            1: [place(0, 1 - xpos), place(1, 1 - xpos), place(1 - ypos, 0), place(1 - ypos, 1)],
            2: [place(1 - ypos, xpos), place(ypos, 1 - xpos)],
            3: [place(ypos, xpos)] * 2,
        }
        tables = {
            key: jnp.stack([jnp.asarray(v, jnp.int32) for v in
                            [2 * pick + (1 - core if key == 0 else core) for pick in value] + list(value)
                            + ([1 - ypos, 1 - xpos] if key == 2 else [ypos, xpos])]).astype(jnp.int32)
            for key, value in picks.items()
        }

        def exchange(value, bit):
            return lax.ppermute(value, "dp", [(i, i ^ bit) for i in range(num_dp)])

        def wgrad(name, number, layer, lhs, rhs, received, pairs, deps, out=None):
            per_half = len(picks[number]) // 2
            steps = 2 * per_half
            own = lhs.shape[2] // num_dp
            cols = rhs.shape[2]
            half = cols // 2
            in_specs = [
                pl.BlockSpec((None, num_groups, own, rows), lambda side, pos, idx: (layer, 0, idx[side * per_half + pos], 0)),
                pl.BlockSpec((None, total, half), lambda side, pos, idx: (layer, 0, side)),
            ]
            inputs = [lhs, rhs]
            if received is not None:
                inputs.append(received)
                in_specs.append(pl.BlockSpec((None, own, half), lambda side, pos, idx: (idx[steps + side * per_half + pos], 0, side)))
            for left, right in pairs:
                inputs += [left, right]
                if left.ndim == 3:
                    in_specs += [pl.BlockSpec((None, own, half), lambda side, pos, idx, which=which: (idx[2 * steps + which], 0, 0))
                                 for which in range(2)]
                else:
                    in_specs += [pl.BlockSpec((own, half), lambda side, pos, idx: (0, 0))] * 2
            aliases = {}
            two_outs = number in (1, 2)
            if number == 0:
                out_shape = [array(steps // 2, own, cols)]
                out_specs = [pl.BlockSpec((None, own, half), lambda side, pos, idx: (pos, 0, side))]
            elif number == 1:
                out_shape = [array(per_half, own, half)] * 2
                out_specs = [pl.BlockSpec((None, own, half), lambda side, pos, idx: (jnp.where(side == 0, pos, per_half - 1), 0, 0)),
                             pl.BlockSpec((None, own, half), lambda side, pos, idx: (jnp.where(side == 0, 0, pos), 0, 0))]
            elif number == 2:
                out_shape = [array(own, half)] * 2
                out_specs = [pl.BlockSpec((own, half), lambda side, pos, idx: (0, 0))] * 2
            else:
                out_shape = [jax.ShapeDtypeStruct((num_layers, own, cols), F32)]
                out_specs = [pl.BlockSpec((None, own, half), lambda side, pos, idx: (layer, 0, side))]
                if out is not None:
                    deps = deps + [out]
                    aliases = {len(inputs) + len(deps): 0}
            return pl.pallas_call(
                functools.partial(wgrad_kernel, len(deps), len(pairs), received is not None, two_outs),
                name=f"wgrad_{name}{layer}_{number}",
                out_shape=out_shape,
                grid_spec=pltpu.PrefetchScalarGridSpec(
                    num_scalar_prefetch=1, grid=(2, per_half),
                    in_specs=in_specs + [any_spec] * len(deps), out_specs=out_specs),
                input_output_aliases=aliases,
                compiler_params=pltpu.CompilerParams(dimension_semantics=("arbitrary", "arbitrary"), vmem_limit_bytes=VMEM_LIMIT),
                cost_estimate=pl.CostEstimate(flops=2 * total * per_half * own * cols, bytes_accessed=2 * total * cols, transcendentals=0),
            )(tables[number], *inputs, *deps)

        final = {}
        last = []

        class Chunk:
            def __init__(self, name, layer, lhs, rhs):
                self.name, self.layer, self.lhs, self.rhs = name, layer, lhs, rhs

            def run(self, number, received=None, pairs=(), out=None):
                res = wgrad(self.name, number, self.layer, acts[self.lhs], grads[self.rhs], received, pairs, list(last), out)
                last[:] = [res[0]]
                return res

            def stage_0(self):
                self.got = exchange(self.run(0)[0], 1)

            def stage_1(self):
                left, right = self.run(1, self.got)
                self.got_1 = (exchange(left, 2), exchange(right, 4))

            def stage_2(self):
                left, right = self.run(2, self.got, [self.got_1])
                self.got_2 = (exchange(left, 4), exchange(right, 2))

            def stage_3(self):
                final[self.name] = self.run(3, self.got, [self.got_1, self.got_2], final.get(self.name))[0]

        recv_fwd = recv_bwd = jnp.zeros((rows, width), BF16)
        acts = grads = None
        dep = recv_fwd
        for tick in range(num_groups + 2):
            if tick <= num_groups:
                send_fwd, acts = forward(slot_idx(tick - stage, stage == 0), recv_fwd, dep, acts)
                if tick < num_groups:
                    recv_fwd = lax.ppermute(send_fwd, "pp", [(0, 1)])
            if 1 <= tick <= num_groups:
                dep, grads = backward(slot_idx(tick - 2 + stage, stage == 1), recv_bwd, acts, grads, num_layers - 1, num_layers)
                recv_bwd = lax.ppermute(dep, "pp", [(1, 0)])

        idx = slot_idx(num_groups - 1 + stage, stage == 1)
        chunks = []
        d_hid = recv_bwd
        for layer in reversed(range(num_layers)):
            if last:
                d_hid = lax.optimization_barrier((d_hid, *last))[0]
            d_hid, grads = backward(idx, d_hid, acts, grads, layer, 1)
            idx = idx * jnp.array([1, 0], jnp.int32)
            make = lambda name, lhs, rhs: Chunk(name, layer, lhs, rhs)
            new = [make("down", "et", "dh2"), make("up", "ct", "du"), make("qkv", "at", "dqkv"), make("out", "ot", "dh1")]
            chunks.append(new)
            if layer == num_layers - 1:
                for chunk in new[:2]:
                    chunk.stage_0()
                for chunk in new[:2]:
                    chunk.stage_1()
        upper, lower = chunks
        order = upper[:2] + lower[:2] + [upper[2], lower[2], upper[3], lower[3]]
        for step in range(2, len(order) + 3):
            for lag, number in ((0, 0), (2, 2), (1, 1), (3, 3)):
                if 0 <= step - lag < len(order) and not (number == 1 and step == 2):
                    getattr(order[step - lag], f"stage_{number}")()

        y_own = acts["h"][num_layers]
        y_recv = lax.ppermute(y_own, "pp", [(1, 0)])
        y_full = jnp.where(stage == 0, y_recv, y_own)
        return (y_full.reshape(x_in.shape), final["qkv"], final["out"], final["up"], final["down"])

    act_spec = P(None, "dp")
    weight_spec = P("pp")
    grad_spec = P("pp", "dp")
    return jax.shard_map(
        device_step,
        mesh=mesh,
        in_specs=(act_spec, act_spec, weight_spec, weight_spec, weight_spec, weight_spec),
        out_specs=(act_spec, grad_spec, grad_spec, grad_spec, grad_spec),
        check_vma=False,
    )
```

```python
import functools

import jax
import jax.numpy as jnp
from jax import lax
from jax.experimental import pallas as pl
from jax.experimental.pallas import tpu as pltpu
from jax.sharding import PartitionSpec as P

HEAD_DIM = 64
NORM_EPS = 1e-6
GROUP = 2
PARTS = 5
SEQ = 128
LANES = 128
BATCHED = 4
F32 = jnp.float32
BF16 = jnp.bfloat16
GELU_A = 0.7978845608028654
GELU_B = 0.044715
VMEM_LIMIT = 67043328
COST = 1000


def dot_nn(lhs, rhs):
    return lax.dot_general(lhs, rhs, (((1,), (0,)), ((), ())), preferred_element_type=F32)


def dot_nt(lhs, rhs):
    return lax.dot_general(lhs, rhs, (((1,), (1,)), ((), ())), preferred_element_type=F32)


def dot_tn(lhs, rhs):
    return lax.dot_general(lhs, rhs, (((0,), (0,)), ((), ())), preferred_element_type=F32)


def inv_rms_of(h_f32):
    return lax.rsqrt(jnp.mean(h_f32 * h_f32, axis=-1, keepdims=True) + NORM_EPS)


def rms_backward(h_f32, grad_f32):
    inv_rms = inv_rms_of(h_f32)
    normed = h_f32 * inv_rms
    return inv_rms * (grad_f32 - normed * jnp.mean(grad_f32 * normed, axis=-1, keepdims=True))


def stack_heads(pair):
    lane = lax.broadcasted_iota(jnp.int32, (1, LANES), 1)
    lo = jnp.where(lane < HEAD_DIM, 1.0, 0.0)
    return jnp.concatenate([pair * lo.astype(BF16), pair * (1.0 - lo).astype(BF16)], axis=0)


def merge_heads(stacked):
    lane = lax.broadcasted_iota(jnp.int32, (SEQ, LANES), 1)
    return jnp.where(lane < HEAD_DIM, stacked[:SEQ], stacked[SEQ:])


def probs_of(scores_t):
    key = lax.broadcasted_iota(jnp.int32, scores_t[0].shape, 0)
    query = jnp.bitwise_and(lax.broadcasted_iota(jnp.int32, scores_t[0].shape, 1), SEQ - 1)
    allowed = key <= query
    masked = [jnp.where(allowed, s * HEAD_DIM ** -0.5, -1e30) for s in scores_t]
    tops = [jnp.max(s, axis=0, keepdims=True) for s in masked]
    exps = [jnp.exp(s - top) for s, top in zip(masked, tops)]
    scales = [1.0 / jnp.sum(e, axis=0, keepdims=True) for e in exps]
    return [e * scale for e, scale in zip(exps, scales)]


def batches(num_rows, num_cols):
    combos = [(seq * SEQ, pair * LANES) for seq in range(num_rows // SEQ) for pair in range(num_cols // LANES)]
    return [combos[pos:pos + BATCHED] for pos in range(0, len(combos), BATCHED)]


def cols_of(part, size, base=0):
    return pl.ds(pl.multiple_of(base + part * size, LANES), size)


def weight_stream(weights, bufs, sems, turn, step, num_turns, layer_of):
    def copy(phase, at, part):
        size = bufs[phase].shape[1]
        slot = lax.rem(part, 3)
        return pltpu.make_async_copy(
            weights[phase].at[layer_of(at), pl.ds(pl.multiple_of(part * size, size), size)], bufs[phase].at[slot], sems.at[phase, slot])

    @pl.when((turn == 0) & (step == 0))
    def _():
        for part in range(2):
            copy(0, turn, jnp.int32(part)).start()

    ahead = step + 2
    at = turn + ahead // (4 * PARTS)
    ahead = lax.rem(ahead, 4 * PARTS)
    for phase in range(4):
        @pl.when((at < num_turns) & (ahead // PARTS == phase))
        def _():
            copy(phase, at, lax.rem(ahead, PARTS)).start()

    def wait(phase, part):
        copy(phase, turn, part).wait()
        return bufs[phase].at[lax.rem(part, 3)]

    return wait


def first_in(own_any, recv_any, dst, idx_ref, row0, sem):
    own = pltpu.make_async_copy(own_any.at[pl.ds(row0, dst.shape[0])], dst, sem)
    recv = pltpu.make_async_copy(recv_any, dst, sem)

    @pl.when(idx_ref[1] == 1)
    def _():
        own.start()
        own.wait()

    @pl.when(idx_ref[1] != 1)
    def _():
        recv.start()
        recv.wait()


def fwd_kernel(n_old, names, idx_ref, *refs):
    x_any, recv_any = refs[:2]
    weights = refs[2:6]
    refs = list(refs[7 + n_old:])
    outs = {name: refs.pop(0) for name in names}
    send_out = refs.pop(0)
    hacc, big, norm, at_scr, ot_scr, qkv_scr, h_scr, u_scr, et_scr, sems, *bufs, w_sems = refs
    rows, width = hacc.shape
    head_cols, hid_cols = width // PARTS, u_scr.shape[1] // PARTS
    layer, step = pl.program_id(0), pl.program_id(1)
    last_layer = pl.num_programs(0) - 1
    row0 = pl.multiple_of(idx_ref[0] * rows, rows)
    sem_of = {name: pos for pos, name in enumerate(names)}

    def whole(name, src, at):
        return pltpu.make_async_copy(src, outs[name].at[at, pl.ds(row0, rows)], sems.at[sem_of[name]])

    def flipped(name, src):
        return pltpu.make_async_copy(src, outs[name].at[layer, idx_ref[0]], sems.at[sem_of[name]])

    def tile(part):
        cols = cols_of(part, hid_cols)
        return pltpu.make_async_copy(u_scr.at[:, cols], outs["u"].at[layer, pl.ds(row0, rows), cols], sems.at[len(names) + 1 + part])

    def again(copy):
        @pl.when(layer > 0)
        def _():
            copy.wait()

    part = lax.rem(step, PARTS)
    phase = step // PARTS

    weight = weight_stream(weights, bufs, w_sems, layer, step, pl.num_programs(0), lambda at: at)

    @pl.when((step == 0) & (layer == 0))
    def _():
        first_in(x_any, recv_any, h_scr, idx_ref, row0, sems.at[sem_of["h"]])
        hacc[...] = h_scr[...].astype(F32)
        whole("h", h_scr, 0).start()

    @pl.when(step == 0)
    def _():
        again(flipped("ct", at_scr))
        h_f32 = hacc[...]
        norm[...] = (h_f32 * inv_rms_of(h_f32)).astype(BF16)
        big[:, :3 * width] = jnp.zeros((rows, 3 * width), F32)

    @pl.when(phase == 0)
    def _():
        a_cols = norm[:, cols_of(part, head_cols)]
        at_scr[cols_of(part, head_cols), :] = a_cols.T
        big[:, :3 * width] += dot_nn(a_cols, weight(0, part)[...])

    @pl.when(step == PARTS)
    def _():
        again(whole("qkv", qkv_scr, layer))
        again(flipped("ot", ot_scr))
        flipped("at", at_scr).start()
        qkv_scr[...] = big[:, :3 * width].astype(BF16)
        whole("qkv", qkv_scr, layer).start()

    @pl.when(phase == 1)
    def _():
        q = qkv_scr[:, cols_of(part, head_cols)]
        k = qkv_scr[:, cols_of(part, head_cols, width)]
        v = qkv_scr[:, cols_of(part, head_cols, 2 * width)]
        pieces = {}
        for batch in batches(rows, head_cols):
            cut = lambda value: [value[r:r + SEQ, c:c + LANES] for r, c in batch]
            scores = [dot_nt(kp, stack_heads(qp)) for qp, kp in zip(cut(q), cut(k))]
            probs = [p.astype(BF16) for p in probs_of(scores)]
            for at, p, vp in zip(batch, probs, cut(v)):
                pieces[at] = merge_heads(dot_tn(p, vp)).astype(BF16)
        o = jnp.concatenate(
            [jnp.concatenate([pieces[r, c] for c in range(0, head_cols, LANES)], axis=1) for r in range(0, rows, SEQ)], axis=0)
        ot_scr[cols_of(part, head_cols), :] = o.T
        hacc[...] += dot_nn(o, weight(1, part)[...])

    @pl.when(step == 2 * PARTS - 1)
    def _():
        whole("h", h_scr, layer).wait()
        flipped("ot", ot_scr).start()
        h_scr[...] = hacc[...].astype(BF16)
        hacc[...] = h_scr[...].astype(F32)
        whole("h1", h_scr, layer).start()

    @pl.when(step == 2 * PARTS)
    def _():
        flipped("at", at_scr).wait()
        h_f32 = hacc[...]
        norm[...] = (h_f32 * inv_rms_of(h_f32)).astype(BF16)
        big[...] = jnp.zeros_like(big)

    @pl.when(phase == 2)
    def _():
        c_cols = norm[:, cols_of(part, head_cols)]
        at_scr[cols_of(part, head_cols), :] = c_cols.T
        big[...] += dot_nn(c_cols, weight(2, part)[...])

    @pl.when(step == 3 * PARTS)
    def _():
        again(flipped("et", et_scr))
        flipped("ct", at_scr).start()

    @pl.when(phase == 3)
    def _():
        again(tile(part))
        sub = 256
        pieces = []
        for pos in range(hid_cols // sub):
            cols = pl.ds(pl.multiple_of(part * hid_cols + pos * sub, LANES), sub)
            up_act = big[:, cols].astype(BF16)
            u_scr[:, cols] = up_act
            u = up_act.astype(F32)
            gelu = u * (0.5 * (1.0 + jnp.tanh(GELU_A * (u + GELU_B * (u * u * u)))))
            pieces.append(gelu.astype(BF16))
            et_scr[cols, :] = pieces[-1].T
        tile(part).start()
        hacc[...] += dot_nn(jnp.concatenate(pieces, axis=1), weight(3, part)[...])

    @pl.when(step == 4 * PARTS - 1)
    def _():
        whole("h1", h_scr, layer).wait()
        h_scr[...] = hacc[...].astype(BF16)
        hacc[...] = h_scr[...].astype(F32)
        whole("h", h_scr, layer + 1).start()

        @pl.when(layer < last_layer)
        def _():
            flipped("et", et_scr).start()

        @pl.when(layer == last_layer)
        def _():
            send = pltpu.make_async_copy(h_scr, send_out, sems.at[len(names)])
            send.start()
            flipped("et", et_scr).start()
            for name, src in (("qkv", qkv_scr), ("h", h_scr)):
                whole(name, src, layer).wait()
            for name, src in (("ot", ot_scr), ("ct", at_scr), ("et", et_scr)):
                flipped(name, src).wait()
            for pos in range(PARTS):
                tile(pos).wait()
            send.wait()


def bwd_kernel(top, n_old, names, idx_ref, *refs):
    seed_any, recv_any, u_any, h_any, h1_any, qkv_any = refs[:6]
    weights = refs[6:10][::-1]
    refs = list(refs[10 + n_old:])
    outs = {name: refs.pop(0) for name in names}
    send_out = refs.pop(0)
    dacc, d_scr, dh1_scr, du_scr, dqkv_scr, qkv_scr, h_scr, h1_scr, sems, in_sems, *bufs, w_sems = refs
    rows, width = dacc.shape
    head_cols, hid_cols = width // PARTS, du_scr.shape[1] // PARTS
    turn, step = pl.program_id(0), pl.program_id(1)
    last_turn = pl.num_programs(0) - 1
    layer = top - turn
    row0 = pl.multiple_of(idx_ref[0] * rows, rows)
    sem_of = {name: pos for pos, name in enumerate(names)}

    def whole(name, src, at):
        return pltpu.make_async_copy(src, outs[name].at[at, pl.ds(row0, rows)], sems.at[sem_of[name]])

    def load(pos, src, dst):
        return pltpu.make_async_copy(src.at[layer, pl.ds(row0, rows)], dst, in_sems.at[pos])

    def again(copy):
        @pl.when(turn > 0)
        def _():
            copy.wait()

    part = lax.rem(step, PARTS)
    phase = step // PARTS

    weight = weight_stream(weights, bufs, w_sems, turn, step, pl.num_programs(0), lambda at: top - at)

    def load_u(at):
        return pltpu.make_async_copy(u_any.at[at, pl.ds(row0, rows)], du_scr, in_sems.at[3])

    @pl.when(step == 0)
    def _():
        @pl.when(turn == 0)
        def _():
            load_u(layer).start()
            first_in(seed_any, recv_any, d_scr, idx_ref, row0, sems.at[sem_of["dh2"]])
            whole("dh2", d_scr, layer).start()

        load(0, h1_any, h1_scr).start()
        load(1, qkv_any, qkv_scr).start()
        load(2, h_any, h_scr).start()
        load_u(layer).wait()

    @pl.when(phase == 0)
    def _():
        sub = 256
        d_out = d_scr[...]
        wdown = weight(0, part)
        for pos in range(hid_cols // sub):
            d_gelu = dot_nt(d_out, wdown[pos * sub:(pos + 1) * sub, :])
            cols = pl.ds(pl.multiple_of(part * hid_cols + pos * sub, LANES), sub)
            u = du_scr[:, cols].astype(F32)
            u2 = u * u
            t = jnp.tanh(GELU_A * (u + GELU_B * (u2 * u)))
            slope = 0.5 * (1.0 + t) + (0.5 * u) * (1.0 - t * t) * (GELU_A + (3.0 * GELU_A * GELU_B) * u2)
            du_scr[:, cols] = (d_gelu * slope).astype(BF16)

    @pl.when(step == PARTS)
    def _():
        whole("du", du_scr, layer).start()

    @pl.when(phase == 1)
    def _():
        dacc[:, cols_of(part, width // PARTS)] = dot_nt(du_scr[...], weight(1, part)[...])

    @pl.when(step == 2 * PARTS - 1)
    def _():
        load(0, h1_any, h1_scr).wait()
        again(whole("dh1", dh1_scr, layer))
        back = rms_backward(h1_scr[...].astype(F32), dacc[...])
        dh1_scr[...] = (d_scr[...].astype(F32) + back).astype(BF16)
        whole("dh1", dh1_scr, layer).start()

    @pl.when(step == 2 * PARTS)
    def _():
        load(1, qkv_any, qkv_scr).wait()
        again(whole("dqkv", dqkv_scr, layer))

    @pl.when(phase == 2)
    def _():
        d_attn = dot_nt(dh1_scr[...], weight(2, part)[...]).astype(BF16)
        q = qkv_scr[:, cols_of(part, head_cols)]
        k = qkv_scr[:, cols_of(part, head_cols, width)]
        v = qkv_scr[:, cols_of(part, head_cols, 2 * width)]
        pieces = ({}, {}, {})
        for batch in batches(rows, head_cols):
            cut = lambda value: [value[r:r + SEQ, c:c + LANES] for r, c in batch]
            q_stacks = [stack_heads(value) for value in cut(q)]
            do_stacks = [stack_heads(value) for value in cut(d_attn)]
            k_pairs = cut(k)
            probs = probs_of([dot_nt(kp, qs) for kp, qs in zip(k_pairs, q_stacks)])
            d_probs = [dot_nt(vp, ds) for vp, ds in zip(cut(v), do_stacks)]
            sums = [jnp.sum(p * dp, axis=0, keepdims=True) for p, dp in zip(probs, d_probs)]
            d_scores = [(p * (dp - s) * HEAD_DIM ** -0.5).astype(BF16) for p, dp, s in zip(probs, d_probs, sums)]
            for pos, at in enumerate(batch):
                pieces[0][at] = merge_heads(dot_tn(d_scores[pos], k_pairs[pos])).astype(BF16)
                pieces[1][at] = dot_nn(d_scores[pos], q_stacks[pos]).astype(BF16)
                pieces[2][at] = dot_nn(probs[pos].astype(BF16), do_stacks[pos]).astype(BF16)
        for third in range(3):
            dqkv_scr[:, cols_of(part, head_cols, third * width)] = jnp.concatenate(
                [jnp.concatenate([pieces[third][r, c] for c in range(0, head_cols, LANES)], axis=1) for r in range(0, rows, SEQ)], axis=0)

    @pl.when(step == 3 * PARTS)
    def _():
        whole("dqkv", dqkv_scr, layer).start()

        @pl.when(turn < last_turn)
        def _():
            whole("du", du_scr, layer).wait()
            load_u(layer - 1).start()

    @pl.when(phase == 3)
    def _():
        dacc[:, cols_of(part, width // PARTS)] = dot_nt(dqkv_scr[...], weight(3, part)[...])

    @pl.when(step == 4 * PARTS - 1)
    def _():
        load(2, h_any, h_scr).wait()

        @pl.when(turn == 0)
        def _():
            whole("dh2", d_scr, layer).wait()

        back = rms_backward(h_scr[...].astype(F32), dacc[...])
        d_scr[...] = (dh1_scr[...].astype(F32) + back).astype(BF16)

        @pl.when(turn < last_turn)
        def _():
            copy = whole("dh2", d_scr, layer - 1)
            copy.start()
            copy.wait()

        @pl.when(turn == last_turn)
        def _():
            send = pltpu.make_async_copy(d_scr, send_out, sems.at[len(names)])
            send.start()
            for name, src in (("du", du_scr), ("dh1", dh1_scr), ("dqkv", dqkv_scr)):
                whole(name, src, layer).wait()
            send.wait()


def wgrad_kernel(number, layer, own, n_pairs, n_deps, idx_ref, lhs_any, rhs_any, *refs):
    refs = list(refs)
    received = refs.pop(0) if number else None
    pairs = [(refs.pop(0), refs.pop(0)) for _ in range(n_pairs)]
    refs = refs[n_deps:]
    outs = [refs.pop(0) for _ in range(2 if number in (1, 2) else 1)]
    lhs_buf, rhs_buf, rec_buf, pair_buf, out_buf, sems = refs
    num_blocks, num_tiles, tile = lhs_buf.shape[0], rhs_buf.shape[0], rhs_buf.shape[2]
    side_tiles = num_tiles // 2
    half = side_tiles * tile
    per_side = {0: 4, 1: 2, 2: 1, 3: 1}[number]
    copies = []

    def begin(src, dst):
        copy = pltpu.make_async_copy(src, dst, sems.at[len(copies)])
        copy.start()
        copies.append(copy)
        return copy

    def load_rhs(pos):
        return begin(rhs_any.at[layer, :, pl.ds(pos * tile, tile)], rhs_buf.at[pos])

    lhs_in, rhs_in, rec_in, pair_in = [], {}, {}, {}
    for block in range(num_blocks):
        lhs_in.append(begin(lhs_any.at[layer, :, pl.ds(pl.multiple_of(idx_ref[block] * own, own), own)], lhs_buf.at[block]))
    rhs_in[0] = load_rhs(0)
    sides = (0, 1) if number else (0,)
    if number:
        rec_base = 2 * per_side
        for side in sides:
            for pos in range(per_side):
                at = side * per_side + pos
                rec_in[at] = begin(received.at[idx_ref[rec_base + at], :, pl.ds(side * half, half)], rec_buf.at[at])
            for which, pair in enumerate(pairs):
                src = pair[side] if len(pair[side].shape) == 2 else pair[side].at[idx_ref[2 * rec_base + side]]
                pair_in[side, which] = begin(src, pair_buf.at[2 * which + side])
    for pos in range(1, num_tiles):
        rhs_in[pos] = load_rhs(pos)
    for copy in lhs_in:
        copy.wait()

    def rows_of(block):
        return jnp.concatenate([lhs_buf[block, group] for group in range(lhs_buf.shape[1])], axis=1)

    leaving = []
    for pos in range(num_tiles):
        side = pos // side_tiles if number else 0
        inner = pos - side * side_tiles if number else pos
        at = [side * per_side + place for place in range(per_side)]
        blocks = [0] if num_blocks == 1 else at
        rhs_in[pos].wait()
        if number and inner == 0:
            for place in at:
                rec_in[place].wait()
            for which in range(n_pairs):
                pair_in[side, which].wait()
        joined = [blocks] if own < 320 else [[block] for block in blocks]
        cols = slice(inner * tile, (inner + 1) * tile)
        for group in joined:
            out = dot_nn(jnp.concatenate([rows_of(block) for block in group], axis=0) if len(group) > 1 else rows_of(group[0]), rhs_buf[pos])
            for order, block in enumerate(group):
                place = blocks.index(block)
                piece = out[order * own:(order + 1) * own]
                if number:
                    piece = piece + rec_buf[at[place], :, cols].astype(F32)
                for which in range(n_pairs):
                    piece = piece + pair_buf[2 * which + side, :, cols].astype(F32)
                out_buf[pos, place] = piece.astype(out_buf.dtype)
                wide = pl.ds((pos if number in (0, 3) else inner) * tile, tile)
                ref = outs[side] if number in (1, 2) else outs[0]
                dst = {0: lambda: ref.at[place, :, wide], 1: lambda: ref.at[place, :, wide], 2: lambda: ref.at[:, wide],
                       3: lambda: ref.at[layer, :, wide]}[number]()
                leaving.append(begin(out_buf.at[pos, place], dst))
    for copy in leaving:
        copy.wait()


def solution(mesh):
    assert mesh.shape["pp"] == 2
    num_dp = mesh.shape["dp"]

    def device_step(x_in, seed_grad, w_qkv, w_out, w_up, w_down):
        num_micro, batch_rows, seq_len, width = x_in.shape
        num_layers = w_qkv.shape[0]
        hidden = w_up.shape[2]
        total = num_micro * batch_rows * seq_len
        rows = GROUP * batch_rows * seq_len
        num_groups = num_micro // GROUP
        stage = lax.axis_index("pp")
        x_rows = x_in.reshape(total, width)
        g_rows = seed_grad.reshape(total, width)
        any_spec = pl.BlockSpec(memory_space=pl.ANY)
        one = jax.ShapeDtypeStruct((rows, width), BF16)

        vmem = lambda *shape: pltpu.VMEM(shape, BF16)

        def array(*shape):
            return jax.ShapeDtypeStruct(shape, BF16)

        def weight_scratch(weights):
            return [vmem(3, weight.shape[1] // PARTS, weight.shape[2]) for weight in weights] + [pltpu.SemaphoreType.DMA((4, 3))]

        def slot_call(body, name, turns, idx, inputs, old, names, shapes, scratch):
            old = [] if old is None else [old[key] for key in names]
            res = pl.pallas_call(
                functools.partial(body, len(old), names),
                name=name,
                out_shape=[shapes[key] for key in names] + [one],
                grid_spec=pltpu.PrefetchScalarGridSpec(
                    num_scalar_prefetch=1,
                    grid=(turns, 4 * PARTS),
                    in_specs=[any_spec] * (len(inputs) + len(old)),
                    out_specs=[any_spec] * (len(names) + 1),
                    scratch_shapes=scratch,
                ),
                input_output_aliases={1 + len(inputs) + pos: pos for pos in range(len(old))},
                compiler_params=pltpu.CompilerParams(
                    dimension_semantics=("arbitrary", "arbitrary"), vmem_limit_bytes=VMEM_LIMIT),
                cost_estimate=pl.CostEstimate(flops=COST, bytes_accessed=COST, transcendentals=0),
            )(idx, *inputs, *old)
            return res[-1], dict(zip(names, res))

        fwd_shapes = {
            "h": array(num_layers + 1, total, width), "at": array(num_layers, num_groups, width, rows),
            "qkv": array(num_layers, total, 3 * width), "ot": array(num_layers, num_groups, width, rows),
            "h1": array(num_layers, total, width), "ct": array(num_layers, num_groups, width, rows),
            "u": array(num_layers, total, hidden), "et": array(num_layers, num_groups, hidden, rows),
        }
        bwd_shapes = {
            "dh2": array(num_layers, total, width), "du": array(num_layers, total, hidden),
            "dh1": array(num_layers, total, width), "dqkv": array(num_layers, total, 3 * width),
        }

        def forward(idx, recv, dep, old):
            inputs = [x_rows, recv, w_qkv, w_out, w_up, w_down, dep]
            scratch = [
                pltpu.VMEM((rows, width), F32), pltpu.VMEM((rows, hidden), F32), vmem(rows, width), vmem(width, rows),
                vmem(width, rows), vmem(rows, 3 * width), vmem(rows, width), vmem(rows, hidden), vmem(hidden, rows), pltpu.SemaphoreType.DMA((len(fwd_shapes) + 1 + PARTS,)),
            ] + weight_scratch(inputs[2:6])
            return slot_call(fwd_kernel, "stage_fwd", num_layers, idx, inputs, old, tuple(fwd_shapes), fwd_shapes, scratch)

        def backward(idx, recv, act, old, top, turns):
            inputs = [g_rows, recv, act["u"], act["h"], act["h1"], act["qkv"], w_qkv, w_out, w_up, w_down]
            scratch = [
                pltpu.VMEM((rows, width), F32), vmem(rows, width), vmem(rows, width), vmem(rows, hidden), vmem(rows, 3 * width),
                vmem(rows, 3 * width), vmem(rows, width), vmem(rows, width),
                pltpu.SemaphoreType.DMA((len(bwd_shapes) + 1,)), pltpu.SemaphoreType.DMA((4,)),
            ] + weight_scratch(inputs[6:][::-1])
            return slot_call(functools.partial(bwd_kernel, top), f"stage_bwd_{top}", turns, idx, inputs, old,
                             tuple(bwd_shapes), bwd_shapes, scratch)

        def slot_idx(group, flag):
            return jnp.stack([jnp.clip(group, 0, num_groups - 1), flag.astype(jnp.int32)]).astype(jnp.int32)

        dp_idx = lax.axis_index("dp")
        core, xpos, ypos = dp_idx % 2, (dp_idx // 2) % 2, dp_idx // 4
        place = lambda y, x: 2 * y + x
        picks = {
            0: [place(0, 0), place(0, 1), place(1, 0), place(1, 1)] * 2,
            1: [place(0, 1 - xpos), place(1, 1 - xpos), place(1 - ypos, 0), place(1 - ypos, 1)],
            2: [place(1 - ypos, xpos), place(ypos, 1 - xpos)],
            3: [place(ypos, xpos)] * 2,
        }
        tables = {
            key: jnp.stack([jnp.asarray(v, jnp.int32) for v in
                            [2 * pick + (1 - core if key == 0 else core) for pick in value] + list(value)
                            + ([1 - ypos, 1 - xpos] if key == 2 else [ypos, xpos])]).astype(jnp.int32)
            for key, value in picks.items()
        }

        def exchange(value, bit):
            return lax.ppermute(value, "dp", [(i, i ^ bit) for i in range(num_dp)])

        def wgrad(name, number, layer, lhs, rhs, received, pairs, deps, out=None):
            own = lhs.shape[2] // num_dp
            cols = rhs.shape[2]
            half = cols // 2
            per_side = len(picks[number]) // 2
            num_blocks = 1 if number == 3 else (4 if number == 0 else 2 * per_side)
            tile = half if half % 1280 else 1280
            num_tiles = cols // tile
            inputs = [lhs, rhs] + ([] if received is None else [received]) + [value for pair in pairs for value in pair]
            aliases = {}
            if number == 0:
                out_shape = [array(4, own, cols)]
            elif number == 1:
                out_shape = [array(2, own, half)] * 2
            elif number == 2:
                out_shape = [array(own, half)] * 2
            else:
                out_shape = [jax.ShapeDtypeStruct((num_layers, own, cols), F32)]
                if out is not None:
                    deps = deps + [out]
                    aliases = {len(inputs) + len(deps): 0}
            places = num_blocks if number == 0 else per_side
            scratch = [
                vmem(num_blocks, num_groups, own, rows), vmem(num_tiles, total, tile),
                vmem(*((2 * per_side, own, half) if number else (1, 16, 128))),
                vmem(*((2 * len(pairs), own, half) if pairs else (1, 16, 128))),
                pltpu.VMEM((num_tiles, places, own, tile), out_shape[0].dtype), pltpu.SemaphoreType.DMA((40,)),
            ]
            return pl.pallas_call(
                functools.partial(wgrad_kernel, number, layer, own, len(pairs), len(deps)),
                name=f"wgrad_{name}{layer}_{number}",
                out_shape=out_shape,
                grid_spec=pltpu.PrefetchScalarGridSpec(
                    num_scalar_prefetch=1, grid=(1,), in_specs=[any_spec] * (len(inputs) + len(deps)),
                    out_specs=[any_spec] * len(out_shape), scratch_shapes=scratch),
                input_output_aliases=aliases,
                compiler_params=pltpu.CompilerParams(dimension_semantics=("arbitrary",), vmem_limit_bytes=VMEM_LIMIT),
                cost_estimate=pl.CostEstimate(flops=COST, bytes_accessed=COST, transcendentals=0),
            )(tables[number], *inputs, *deps)

        final = {}
        last = []

        class Chunk:
            def __init__(self, name, layer, lhs, rhs):
                self.name, self.layer, self.lhs, self.rhs = name, layer, lhs, rhs

            def run(self, number, received=None, pairs=(), out=None):
                res = wgrad(self.name, number, self.layer, acts[self.lhs], grads[self.rhs], received, pairs, list(last), out)
                last[:] = [res[0]]
                return res

            def stage_0(self):
                self.got = exchange(self.run(0)[0], 1)

            def stage_1(self):
                left, right = self.run(1, self.got)
                self.got_1 = (exchange(left, 2), exchange(right, 4))

            def stage_2(self):
                left, right = self.run(2, self.got, [self.got_1])
                self.got_2 = (exchange(left, 4), exchange(right, 2))

            def stage_3(self):
                final[self.name] = self.run(3, self.got, [self.got_1, self.got_2], final.get(self.name))[0]

        recv_fwd = recv_bwd = jnp.zeros((rows, width), BF16)
        acts = grads = None
        dep = recv_fwd
        for tick in range(num_groups + 2):
            if tick <= num_groups:
                send_fwd, acts = forward(slot_idx(tick - stage, stage == 0), recv_fwd, dep, acts)
                if tick < num_groups:
                    recv_fwd = lax.ppermute(send_fwd, "pp", [(0, 1)])
            if 1 <= tick <= num_groups:
                dep, grads = backward(slot_idx(tick - 2 + stage, stage == 1), recv_bwd, acts, grads, num_layers - 1, num_layers)
                recv_bwd = lax.ppermute(dep, "pp", [(1, 0)])

        idx = slot_idx(num_groups - 1 + stage, stage == 1)
        chunks = []
        d_hid = recv_bwd
        for layer in reversed(range(num_layers)):
            if last:
                d_hid = lax.optimization_barrier((d_hid, *last))[0]
            d_hid, grads = backward(idx, d_hid, acts, grads, layer, 1)
            idx = idx * jnp.array([1, 0], jnp.int32)
            make = lambda name, lhs, rhs: Chunk(name, layer, lhs, rhs)
            new = [make("down", "et", "dh2"), make("up", "ct", "du"), make("qkv", "at", "dqkv"), make("out", "ot", "dh1")]
            chunks.append(new)
            if layer == num_layers - 1:
                for chunk in new[:2]:
                    chunk.stage_0()
                for chunk in new[:2]:
                    chunk.stage_1()
        upper, lower = chunks
        order = upper[:2] + lower[:2] + [upper[2], lower[2], upper[3], lower[3]]
        for step in range(2, len(order) + 3):
            for lag, number in ((0, 0), (2, 2), (1, 1), (3, 3)):
                if 0 <= step - lag < len(order) and not (number == 1 and step == 2):
                    getattr(order[step - lag], f"stage_{number}")()

        y_own = acts["h"][num_layers]
        y_recv = lax.ppermute(y_own, "pp", [(1, 0)])
        y_full = jnp.where(stage == 0, y_recv, y_own)
        return (y_full.reshape(x_in.shape), final["qkv"], final["out"], final["up"], final["down"])

    act_spec = P(None, "dp")
    weight_spec = P("pp")
    grad_spec = P("pp", "dp")
    return jax.shard_map(
        device_step,
        mesh=mesh,
        in_specs=(act_spec, act_spec, weight_spec, weight_spec, weight_spec, weight_spec),
        out_specs=(act_spec, grad_spec, grad_spec, grad_spec, grad_spec),
        check_vma=False,
    )
```
